512 devices in a mesh: slab: 128 (over x_lo, z, y), band: 4 (over x_hi, core).
Axes of the slice: x: 4 (x_hi: 2, x_lo: 2; x = x_hi * 2 + x_lo), y: 8, z: 8, core: 2. Of those that a mesh axis runs over, the one named last changes fastest.
Arguments:
- orbitals: float32 [8, 128, 128, 128], P('band', 'slab'), may hold values from -6 to 6
Outputs:
- exchange_out: float32 [8, 128, 128, 128], P('band', 'slab')
The draws below stay inside these ranges and needn't reach their ends.
All inputs are finite; a program needn't handle non-finite values.
Results may differ from the reference program's by a relative error of at most 0.00013.
Values sent between devices are 32-bit elements; how exact they have to be, the bound alone decides.
A program may use at most 64 MiB of HBM per device.

```python
import math
import jax
import jax.numpy as jnp
from jax import lax

NX = 128
NY = 128
NZ = 128
OB = 2
NORB = 8
N_BAND = 4


def block_levels(key, shape, cuts, low, high):
    level, own = 1.0, jax.random.fold_in(key, 6)
    for position, blocks in cuts:
        heights = jnp.exp(jax.random.uniform(jax.random.fold_in(own, position), (blocks,), jnp.float32, low / len(cuts), high / len(cuts)))
        level = level * jnp.repeat(heights, shape[position] // blocks).reshape([-1 if axis == position else 1 for axis in range(len(shape))])
    return level


def bell_draw(rng, dims, spread, limit, cuts=(), held_as=jnp.bfloat16):
    entries = jax.random.normal(rng, dims, jnp.float32) * spread
    if len(cuts) > 0:
        entries = block_levels(rng, dims, cuts, -0.22, 0.18) * entries
    return jnp.clip(entries, min=-limit, max=limit).astype(held_as)


def setup_inputs(seed: int = 0) -> dict:
    key_list = jax.random.split(jax.random.key(seed), 2)
    orbitals = bell_draw(key_list[0], (NORB, NZ, NY, NX), 1.0, 6.0, ((0, 4), (1, 128)), jnp.float32)
    return dict(orbitals=orbitals)


screen_width = 0.5


def frequency(counter, length):
    return jnp.where(counter < length // 2, counter, counter - length).astype(jnp.float32)


def screened(squared):
    safe_sq = jnp.where(squared > 0, squared, 1.0)
    value = 4.0 * math.pi / safe_sq * (1.0 - jnp.exp(-safe_sq / (4.0 * screen_width ** 2)))
    return jnp.where(squared > 0, value, math.pi / screen_width ** 2)


def kernel_half():
    freq_z = frequency(jnp.arange(NZ, dtype=jnp.int32), NZ)
    freq_y = frequency(jnp.arange(NY, dtype=jnp.int32), NY)
    freq_x = jnp.arange(NX // 2 + 1, dtype=jnp.int32).astype(jnp.float32)
    squared = ((2.0 * math.pi / NZ) * freq_z) ** 2
    squared = squared[:, None, None] + (((2.0 * math.pi / NY) * freq_y) ** 2)[None, :, None]
    squared = squared + (((2.0 * math.pi / NX) * freq_x) ** 2)[None, None, :]
    return screened(squared)


def reference(orbitals):
    blocks = orbitals.reshape(N_BAND, OB, NZ, NY, NX)
    partner = jnp.roll(blocks, 1, axis=0)
    weights = kernel_half()

    def one_block(pair_args):
        own_block, other_block = pair_args
        partners = jnp.concatenate([own_block, other_block], axis=0)

        def one_target(target):
            def add_term(accum, partner_orb):
                density = target * partner_orb
                spectrum = jnp.fft.rfftn(density, axes=(0, 1, 2))
                potential = jnp.fft.irfftn(weights * spectrum, s=(NZ, NY, NX), axes=(0, 1, 2))
                return accum + potential * partner_orb, None

            accum, unused = lax.scan(add_term, jnp.zeros_like(target), partners)
            return -accum

        return lax.map(one_target, own_block)

    result = lax.map(one_block, (blocks, partner))
    return result.reshape(NORB, NZ, NY, NX)
```

```python
import functools
import math

import jax
import jax.numpy as jnp
import numpy as np
from jax import lax
from jax.experimental import pallas as pl
from jax.experimental.pallas import tpu as pltpu
from jax.sharding import PartitionSpec as P

screen_width = 0.5
N = 128
BANDS = 4
LOGICAL = pl.DeviceIdType.LOGICAL
CHUNKS = ((0, 3), (3, 4))


def basis():
    row = np.arange(N)
    freq = np.where(row <= N // 2, row, row - N // 2)
    angle = 2.0 * np.pi / N * ((freq[:, None] * row[None, :]) % N)
    table = np.where(row[:, None] <= N // 2, np.cos(angle), np.sin(angle)) * np.sqrt(2.0 / N)
    table[0] *= np.sqrt(0.5)
    table[N // 2] *= np.sqrt(0.5)
    high = table.astype(np.float32).astype(jnp.bfloat16)
    low = (table - high.astype(np.float64)).astype(np.float32).astype(jnp.bfloat16)
    return np.stack([high, low, high.T, low.T])


def offsets():
    ring = lambda d: min(d, 8 - d)
    steps = [(dx, dz, dy) for dx in range(2) for dz in range(8) for dy in range(8)]
    steps.remove((0, 0, 0))
    return sorted(steps, key=lambda s: -(s[0] + ring(s[1]) + ring(s[2])))


def split(value):
    high = value.astype(jnp.bfloat16)
    return high, (value - high.astype(jnp.float32)).astype(jnp.bfloat16)


def times(value, right):
    both = jnp.dot(jnp.concatenate(split(value), axis=1), right, preferred_element_type=jnp.float32)
    return both[:, :N] + both[:, N:]


def applied(left, value):
    both = jnp.dot(left, jnp.concatenate(split(value), axis=0), preferred_element_type=jnp.float32)
    return both[:N] + both[N:]


def screened(squared):
    safe_sq = jnp.where(squared > 0, squared, 1.0)
    value = 4.0 * math.pi / safe_sq * (1.0 - jnp.exp(-safe_sq / (4.0 * screen_width**2)))
    return jnp.where(squared > 0, value, math.pi / screen_width**2)


def squares(index):
    freq = jnp.where(index <= N // 2, index, index - N // 2).astype(jnp.float32)
    return (2.0 * math.pi / N * freq) ** 2


def kernel(
    orb_hbm, basis_hbm, out_ref, own, other, tables, out1, in1, out2, in2, weight,
    load_sem, near_send, near_recv, send_sem, recv_sem,
):
    me, band = lax.axis_index("slab"), lax.axis_index("band")
    x, z, y = lax.div(me, 64), lax.rem(lax.div(me, 8), 8), lax.rem(me, 8)
    at_x = [lax.rem(x + d, 2) * (64 * BANDS) + band for d in range(2)]
    at_z = [lax.rem(z + d, 8) * (8 * BANDS) for d in range(8)]
    at_y = [lax.rem(y + d, 8) * BANDS for d in range(8)]
    peers = [(lax.rem(x + dx, 2) * 64 + lax.rem(z + dz, 8) * 8 + lax.rem(y + dy, 8), at_x[dx] + at_z[dz] + at_y[dy]) for dx, dz, dy in offsets()]
    following = me * BANDS + lax.rem(band + 1, BANDS)
    previous = me * BANDS + lax.rem(band + BANDS - 1, BANDS)

    load_own = pltpu.make_async_copy(orb_hbm, own, load_sem.at[0])
    load_tables = pltpu.make_async_copy(basis_hbm, tables, load_sem.at[1])
    load_own.start()
    load_tables.start()

    barrier = pltpu.get_barrier_semaphore()
    for _, device in peers:
        pl.semaphore_signal(barrier, inc=1, device_id=device, device_id_type=LOGICAL)
    pl.semaphore_signal(barrier, inc=1, device_id=previous, device_id_type=LOGICAL)

    def sends(source, target, number):
        first, rows = CHUNKS[number % 2]
        for slab, device in peers:
            pltpu.make_async_remote_copy(
                src_ref=source.at[slab, pl.ds(first, rows)],
                dst_ref=target.at[me, pl.ds(first, rows)],
                send_sem=send_sem.at[number],
                recv_sem=recv_sem.at[number],
                device_id=device,
                device_id_type=LOGICAL,
            ).start()
        target[me, pl.ds(first, rows)] = source[me, pl.ds(first, rows)]

    def whole(source, target, number):
        first, rows = CHUNKS[number % 2]
        return pltpu.make_async_remote_copy(
            src_ref=source.at[pl.ds(0, N - 1), pl.ds(first, rows)],
            dst_ref=target.at[pl.ds(0, N - 1), pl.ds(first, rows)],
            send_sem=send_sem.at[number],
            recv_sem=recv_sem.at[number],
            device_id=following,
            device_id_type=LOGICAL,
        )

    def gather(ref, chunk):
        first, rows = CHUNKS[chunk]
        flat = ref.reshape(N * 8, N)
        return jnp.concatenate([flat[pl.ds(first + p, N, stride=8), :] for p in range(rows)], axis=1)

    def scatter(ref, chunk, value):
        first, rows = CHUNKS[chunk]
        flat = ref.reshape(N * 8, N)
        for p in range(rows):
            flat[pl.ds(first + p, N, stride=8), :] = value[:, p * N : (p + 1) * N]

    row = lax.broadcasted_iota(jnp.int32, (N, N), 0)
    column = lax.broadcasted_iota(jnp.int32, (N, N), 1)
    weight[...] = screened(squares(row) + squares(jnp.full((N, N), me, jnp.int32)) + squares(column))

    load_own.wait()
    load_tables.wait()
    high, low, high_t, low_t = (tables[i] for i in range(4))

    def right_of(a, b):
        both = jnp.concatenate([a, b], axis=1)
        return jnp.concatenate([both, both], axis=0)

    def left_of(a, b):
        both = jnp.concatenate([a, b], axis=0)
        return jnp.concatenate([both, both], axis=1)

    def forward(chunk, densities):
        first = times(jnp.concatenate(densities, axis=0), right_of(high_t, low_t))
        side = jnp.concatenate([first[p * N : (p + 1) * N] for p in range(len(densities))], axis=1)
        scatter(out1, chunk, applied(left_of(high, low), side))

    def middle(chunk):
        spectrum = applied(left_of(high, low), gather(in1, chunk))
        spectrum = spectrum * jnp.concatenate([weight[...]] * CHUNKS[chunk][1], axis=1)
        scatter(out2, chunk, applied(left_of(high_t, low_t), spectrum))

    def backward(chunk):
        rows = CHUNKS[chunk][1]
        side = applied(left_of(high_t, low_t), gather(in2, chunk))
        stack = jnp.concatenate([side[:, p * N : (p + 1) * N] for p in range(rows)], axis=0)
        field = times(stack, right_of(high, low))
        return [field[p * N : (p + 1) * N] for p in range(rows)]

    forward(0, [own[0] * own[0], own[0] * own[1], own[1] * own[1]])

    pl.semaphore_wait(barrier, N)
    shift = pltpu.make_async_remote_copy(
        src_ref=own, dst_ref=other, send_sem=near_send, recv_sem=near_recv, device_id=following, device_id_type=LOGICAL
    )
    shift.start()
    sends(out1, in1, 0)
    shift.wait_recv()
    forward(1, [own[0] * other[0], own[0] * other[1], own[1] * other[0], own[1] * other[1]])
    sends(out1, in1, 1)
    for chunk in range(2):
        whole(out1, in1, chunk).wait_recv()
        middle(chunk)
        sends(out2, in2, 2 + chunk)
    whole(out2, in2, 2).wait_recv()
    field = backward(0)
    own_part = [field[0] * own[0] + field[1] * own[1], field[1] * own[0] + field[2] * own[1]]
    whole(out2, in2, 3).wait_recv()
    field = backward(1)
    out_ref[0] = -(own_part[0] + (field[0] * other[0] + field[1] * other[1]))
    out_ref[1] = -(own_part[1] + (field[2] * other[0] + field[3] * other[1]))
    shift.wait_send()
    for number in range(4):
        source, target = ((out1, in1), (out2, in2))[number // 2]
        whole(source, target, number).wait_send()


def body(orbitals):
    plane = pltpu.VMEM((N, 8, N), jnp.float32)
    pair = pltpu.VMEM((2, N, N), jnp.float32)
    result = pl.pallas_call(
        kernel,
        out_shape=jax.ShapeDtypeStruct((2, N, N), jnp.float32),
        in_specs=[pl.BlockSpec(memory_space=pl.ANY)] * 2,
        out_specs=pl.BlockSpec(memory_space=pltpu.VMEM),
        scratch_shapes=[
            pair,
            pair,
            pltpu.VMEM((4, N, N), jnp.bfloat16),
            plane,
            plane,
            plane,
            plane,
            pltpu.VMEM((N, N), jnp.float32),
            pltpu.SemaphoreType.DMA((2,)),
            pltpu.SemaphoreType.DMA,
            pltpu.SemaphoreType.DMA,
            pltpu.SemaphoreType.DMA((4,)),
            pltpu.SemaphoreType.DMA((4,)),
        ],
        compiler_params=pltpu.CompilerParams(collective_id=0, has_side_effects=True),
        name="exchange",
    )(orbitals.reshape(2, N, N), jnp.asarray(basis()))
    return result.reshape(orbitals.shape)


def solution(mesh):
    placed = P("band", "slab", None, None)
    return jax.shard_map(body, mesh=mesh, in_specs=(placed,), out_specs=placed, check_vma=False)
```

```python
import functools
import math

import jax
import jax.numpy as jnp
import numpy as np
from jax import lax
from jax.experimental import pallas as pl
from jax.experimental.pallas import tpu as pltpu
from jax.sharding import PartitionSpec as P

screen_width = 0.5
N = 128
BANDS = 4
LOGICAL = pl.DeviceIdType.LOGICAL
CHUNKS = ((0, 3), (3, 4))


def basis():
    row = np.arange(N)
    freq = np.where(row <= N // 2, row, row - N // 2)
    angle = 2.0 * np.pi / N * ((freq[:, None] * row[None, :]) % N)
    table = np.where(row[:, None] <= N // 2, np.cos(angle), np.sin(angle)) * np.sqrt(2.0 / N)
    table[0] *= np.sqrt(0.5)
    table[N // 2] *= np.sqrt(0.5)
    high = table.astype(np.float32).astype(jnp.bfloat16)
    low = (table - high.astype(np.float64)).astype(np.float32).astype(jnp.bfloat16)
    return np.stack([high, low, high.T, low.T])


def offsets():
    ring = lambda d: min(d, 8 - d)
    steps = [(dx, dz, dy) for dx in range(2) for dz in range(8) for dy in range(8)]
    steps.remove((0, 0, 0))
    return sorted(steps, key=lambda s: -(s[0] + ring(s[1]) + ring(s[2])))


def plane_offsets():
    ring = lambda d: min(d, 8 - d)
    steps = [(dx, dy) for dx in range(2) for dy in range(8)]
    return sorted(steps, key=lambda s: -(s[0] + ring(s[1])))


def split(value):
    high = value.astype(jnp.bfloat16)
    return high, (value - high.astype(jnp.float32)).astype(jnp.bfloat16)


def times(value, right):
    both = jnp.dot(jnp.concatenate(split(value), axis=1), right, preferred_element_type=jnp.float32)
    return both[:, :N] + both[:, N:]


def applied(left, value):
    both = jnp.dot(left, jnp.concatenate(split(value), axis=0), preferred_element_type=jnp.float32)
    return both[:N] + both[N:]


def screened(squared):
    safe_sq = jnp.where(squared > 0, squared, 1.0)
    value = 4.0 * math.pi / safe_sq * (1.0 - jnp.exp(-safe_sq / (4.0 * screen_width**2)))
    return jnp.where(squared > 0, value, math.pi / screen_width**2)


def squares(index):
    freq = jnp.where(index <= N // 2, index, index - N // 2).astype(jnp.float32)
    return (2.0 * math.pi / N * freq) ** 2


def kernel(
    orb_hbm, basis_hbm, out_ref, own, other, tables, out1, in1, out2, in2, weight,
    load_sem, near_send, near_recv, send_sem, recv_sem,
):
    load_own = pltpu.make_async_copy(orb_hbm, own, load_sem.at[0])
    load_tables = pltpu.make_async_copy(basis_hbm, tables, load_sem.at[1])
    load_own.start()
    load_tables.start()
    me, band = lax.axis_index("slab"), lax.axis_index("band")
    x, z, y = lax.div(me, 64), lax.rem(lax.div(me, 8), 8), lax.rem(me, 8)
    at_x = [lax.rem(x + d, 2) * (64 * BANDS) + band for d in range(2)]
    at_z = [lax.rem(z + d, 8) * (8 * BANDS) for d in range(8)]
    at_y = [lax.rem(y + d, 8) * BANDS for d in range(8)]
    peers = [(lax.rem(x + dx, 2) * 64 + lax.rem(z + dz, 8) * 8 + lax.rem(y + dy, 8), at_x[dx] + at_z[dz] + at_y[dy]) for dx, dz, dy in offsets()]
    following = me * BANDS + lax.rem(band + 1, BANDS)
    previous = me * BANDS + lax.rem(band + BANDS - 1, BANDS)

    barrier = pltpu.get_barrier_semaphore()
    for _, device in peers:
        pl.semaphore_signal(barrier, inc=1, device_id=device, device_id_type=LOGICAL)
    pl.semaphore_signal(barrier, inc=1, device_id=previous, device_id_type=LOGICAL)

    flat_peers = [(lax.rem(x + dx, 2) * 64 + lax.rem(y + dy, 8), at_x[dx] + at_y[dy]) for dx, dy in plane_offsets()]

    def returns(source, target, number, planes):
        first, rows = CHUNKS[number % 2]
        for plane in planes:
            for index, (slab, device) in enumerate(flat_peers):
                copy = pltpu.make_async_remote_copy(
                    src_ref=source.at[slab + plane * 8, pl.ds(first, rows)],
                    dst_ref=target.at[me, pl.ds(first, rows)],
                    send_sem=send_sem.at[number],
                    recv_sem=recv_sem.at[number],
                    device_id=device + plane * (8 * BANDS),
                    device_id_type=LOGICAL,
                )
                if index == len(flat_peers) - 1:
                    pl.when(z != plane)(copy.start)
                else:
                    copy.start()

    def keep(source, target, number):
        first, rows = CHUNKS[number % 2]
        target[me, pl.ds(first, rows)] = source[me, pl.ds(first, rows)]

    def sends(source, target, number):
        first, rows = CHUNKS[number % 2]
        for slab, device in peers:
            pltpu.make_async_remote_copy(
                src_ref=source.at[slab, pl.ds(first, rows)],
                dst_ref=target.at[me, pl.ds(first, rows)],
                send_sem=send_sem.at[number],
                recv_sem=recv_sem.at[number],
                device_id=device,
                device_id_type=LOGICAL,
            ).start()
        target[me, pl.ds(first, rows)] = source[me, pl.ds(first, rows)]

    def whole(source, target, number):
        first, rows = CHUNKS[number % 2]
        return pltpu.make_async_remote_copy(
            src_ref=source.at[pl.ds(0, N - 1), pl.ds(first, rows)],
            dst_ref=target.at[pl.ds(0, N - 1), pl.ds(first, rows)],
            send_sem=send_sem.at[number],
            recv_sem=recv_sem.at[number],
            device_id=following,
            device_id_type=LOGICAL,
        )

    def gather(ref, chunk):
        first, rows = CHUNKS[chunk]
        flat = ref.reshape(N * 8, N)
        return jnp.concatenate([flat[pl.ds(first + p, N, stride=8), :] for p in range(rows)], axis=1)

    def scatter(ref, chunk, value):
        first, rows = CHUNKS[chunk]
        flat = ref.reshape(N * 8, N)
        for p in range(rows):
            flat[pl.ds(first + p, N, stride=8), :] = value[:, p * N : (p + 1) * N]

    row = lax.broadcasted_iota(jnp.int32, (N, N), 0)
    column = lax.broadcasted_iota(jnp.int32, (N, N), 1)
    weight[...] = screened(squares(row) + squares(jnp.full((N, N), me, jnp.int32)) + squares(column))

    load_own.wait()
    load_tables.wait()
    high, low, high_t, low_t = (tables[i] for i in range(4))

    def right_of(a, b):
        both = jnp.concatenate([a, b], axis=1)
        return jnp.concatenate([both, both], axis=0)

    def left_of(a, b):
        both = jnp.concatenate([a, b], axis=0)
        return jnp.concatenate([both, both], axis=1)

    def forward(chunk, densities):
        first = times(jnp.concatenate(densities, axis=0), right_of(high_t, low_t))
        side = jnp.concatenate([first[p * N : (p + 1) * N] for p in range(len(densities))], axis=1)
        scatter(out1, chunk, applied(left_of(high, low), side))

    def middle(chunk):
        spectrum = applied(left_of(high, low), gather(in1, chunk))
        spectrum = spectrum * jnp.concatenate([weight[...]] * CHUNKS[chunk][1], axis=1)
        scatter(out2, chunk, applied(left_of(high_t, low_t), spectrum))

    def backward(chunk):
        rows = CHUNKS[chunk][1]
        side = applied(left_of(high_t, low_t), gather(in2, chunk))
        stack = jnp.concatenate([side[:, p * N : (p + 1) * N] for p in range(rows)], axis=0)
        field = times(stack, right_of(high, low))
        return [field[p * N : (p + 1) * N] for p in range(rows)]

    forward(0, [own[0] * own[0], own[0] * own[1], own[1] * own[1]])

    pl.semaphore_wait(barrier, N)
    shift = pltpu.make_async_remote_copy(
        src_ref=own, dst_ref=other, send_sem=near_send, recv_sem=near_recv, device_id=following, device_id_type=LOGICAL
    )
    shift.start()
    sends(out1, in1, 0)
    shift.wait_recv()
    forward(1, [own[0] * other[0], own[0] * other[1], own[1] * other[0], own[1] * other[1]])
    sends(out1, in1, 1)
    for chunk in range(2):
        whole(out1, in1, chunk).wait_recv()
        middle(chunk)
        keep(out2, in2, 2 + chunk)
        returns(out2, in2, 2 + chunk, range(8))
    whole(out2, in2, 2).wait_recv()
    field = backward(0)
    own_part = [field[0] * own[0] + field[1] * own[1], field[1] * own[0] + field[2] * own[1]]
    whole(out2, in2, 3).wait_recv()
    field = backward(1)
    out_ref[0] = (own_part[0] + (field[0] * other[0] + field[1] * other[1]))
    out_ref[1] = (own_part[1] + (field[2] * other[0] + field[3] * other[1]))
    shift.wait_send()
    for number in range(4):
        source, target = ((out1, in1), (out2, in2))[number // 2]
        whole(source, target, number).wait_send()


def body(orbitals):
    plane = pltpu.VMEM((N, 8, N), jnp.float32)
    pair = pltpu.VMEM((2, N, N), jnp.float32)
    result = pl.pallas_call(
        kernel,
        out_shape=pltpu.VMEM((2, N, N), jnp.float32),
        in_specs=[pl.BlockSpec(memory_space=pltpu.HBM)] * 2,
        out_specs=pl.BlockSpec(memory_space=pltpu.VMEM),
        scratch_shapes=[
            pair,
            pair,
            pltpu.VMEM((4, N, N), jnp.bfloat16),
            plane,
            plane,
            plane,
            plane,
            pltpu.VMEM((N, N), jnp.float32),
            pltpu.SemaphoreType.DMA((2,)),
            pltpu.SemaphoreType.DMA,
            pltpu.SemaphoreType.DMA,
            pltpu.SemaphoreType.DMA((4,)),
            pltpu.SemaphoreType.DMA((4,)),
        ],
        compiler_params=pltpu.CompilerParams(collective_id=0, has_side_effects=True),
        name="exchange",
    )(orbitals.reshape(2, N, N), jnp.asarray(basis()))
    return -result.reshape(orbitals.shape)


def solution(mesh):
    placed = P("band", "slab", None, None)
    return jax.shard_map(body, mesh=mesh, in_specs=(placed,), out_specs=placed, check_vma=False)
```

```python
import functools
import math

import jax
import jax.numpy as jnp
import numpy as np
from jax import lax
from jax.experimental import pallas as pl
from jax.experimental.pallas import tpu as pltpu
from jax.sharding import PartitionSpec as P

screen_width = 0.5
N = 128
BANDS = 4
LOGICAL = pl.DeviceIdType.LOGICAL
CHUNKS = ((0, 3), (3, 4))


def basis():
    row = np.arange(N)
    freq = np.where(row <= N // 2, row, row - N // 2)
    angle = 2.0 * np.pi / N * ((freq[:, None] * row[None, :]) % N)
    table = np.where(row[:, None] <= N // 2, np.cos(angle), np.sin(angle)) * np.sqrt(2.0 / N)
    table[0] *= np.sqrt(0.5)
    table[N // 2] *= np.sqrt(0.5)
    high = table.astype(np.float32).astype(jnp.bfloat16)
    low = (table - high.astype(np.float64)).astype(np.float32).astype(jnp.bfloat16)
    return np.stack([high, low, high.T, low.T])


def plane_offsets():
    ring = lambda d: min(d, 8 - d)
    steps = [(dx, dy) for dx in range(2) for dy in range(8)]
    return sorted(steps, key=lambda s: -(s[0] + ring(s[1])))


def split(value):
    high = value.astype(jnp.bfloat16)
    return high, (value - high.astype(jnp.float32)).astype(jnp.bfloat16)


def times(value, right):
    both = jnp.dot(jnp.concatenate(split(value), axis=1), right, preferred_element_type=jnp.float32)
    return both[:, :N] + both[:, N:]


def applied(left, value):
    both = jnp.dot(left, jnp.concatenate(split(value), axis=0), preferred_element_type=jnp.float32)
    return both[:N] + both[N:]


def screened(squared):
    safe_sq = jnp.where(squared > 0, squared, 1.0)
    value = 4.0 * math.pi / safe_sq * (1.0 - jnp.exp(-safe_sq / (4.0 * screen_width**2)))
    return jnp.where(squared > 0, value, math.pi / screen_width**2)


def squares(index):
    freq = jnp.where(index <= N // 2, index, index - N // 2).astype(jnp.float32)
    return (2.0 * math.pi / N * freq) ** 2


def kernel(
    orb_hbm, basis_hbm, out_ref, own, other, tables, out1, in1, out2, in2, weight,
    load_sem, near_send, near_recv, send_sem, recv_sem,
):
    load_own = pltpu.make_async_copy(orb_hbm, own, load_sem.at[0])
    load_tables = pltpu.make_async_copy(basis_hbm, tables, load_sem.at[1])
    load_own.start()
    load_tables.start()
    me, band = lax.axis_index("slab"), lax.axis_index("band")
    x, z, y = lax.div(me, 64), lax.rem(lax.div(me, 8), 8), lax.rem(me, 8)
    at_x = [lax.rem(x + d, 2) * (64 * BANDS) + band for d in range(2)]
    at_y = [lax.rem(y + d, 8) * BANDS for d in range(8)]
    following = me * BANDS + lax.rem(band + 1, BANDS)
    previous = me * BANDS + lax.rem(band + BANDS - 1, BANDS)

    def keep(source, target, number):
        first, rows = CHUNKS[number % 2]
        target[me, pl.ds(first, rows)] = source[me, pl.ds(first, rows)]

    flat = [(lax.rem(x + dx, 2) * 64 + lax.rem(y + dy, 8), at_x[dx] + at_y[dy]) for dx, dy in plane_offsets()]
    at_z = [lax.rem(z + d, 8) for d in range(8)]
    rounds = [[at_z[step] for step in steps] for steps in ((4,), (3, 5), (2, 6), (1, 7), (0,))]

    def peers():
        for planes in rounds:
            for slab, device in flat[:-1] if planes is rounds[-1] else flat:
                for plane in planes:
                    yield slab + plane * 8, device + plane * (8 * BANDS)

    def copy_to(source, target, number, slab, device):
        first, rows = CHUNKS[number % 2]
        return pltpu.make_async_remote_copy(
            src_ref=source.at[slab, pl.ds(first, rows)],
            dst_ref=target.at[me, pl.ds(first, rows)],
            send_sem=send_sem.at[number],
            recv_sem=recv_sem.at[number],
            device_id=device,
            device_id_type=LOGICAL,
        )

    def sends(source, target, number):
        for slab, device in peers():
            copy_to(source, target, number, slab, device).start()
        keep(source, target, number)

    def returns(source, target, number):
        for plane in range(8):
            for row in (0, 1, 2, 7, 3, 6, 4, 5):
                for step in (1, 0):
                    slab = lax.rem(x + step, 2) * 64 + plane * 8 + row
                    out_copy = copy_to(source, target, number, slab, at_x[step] + (plane * 8 + row) * BANDS)
                    if step == 1:
                        out_copy.start()
                    else:
                        pl.when(slab != me)(out_copy.start)
        keep(source, target, number)

    barrier = pltpu.get_barrier_semaphore()
    for _, device in peers():
        pl.semaphore_signal(barrier, inc=1, device_id=device, device_id_type=LOGICAL)
    pl.semaphore_signal(barrier, inc=1, device_id=previous, device_id_type=LOGICAL)

    def whole(source, target, number):
        first, rows = CHUNKS[number % 2]
        return pltpu.make_async_remote_copy(
            src_ref=source.at[pl.ds(0, N - 1), pl.ds(first, rows)],
            dst_ref=target.at[pl.ds(0, N - 1), pl.ds(first, rows)],
            send_sem=send_sem.at[number],
            recv_sem=recv_sem.at[number],
            device_id=following,
            device_id_type=LOGICAL,
        )

    def gather(ref, chunk):
        first, rows = CHUNKS[chunk]
        flat = ref.reshape(N * 8, N)
        return jnp.concatenate([flat[pl.ds(first + p, N, stride=8), :] for p in range(rows)], axis=1)

    def scatter(ref, chunk, value):
        first, rows = CHUNKS[chunk]
        flat = ref.reshape(N * 8, N)
        for p in range(rows):
            flat[pl.ds(first + p, N, stride=8), :] = value[:, p * N : (p + 1) * N]

    row = lax.broadcasted_iota(jnp.int32, (N, N), 0)
    column = lax.broadcasted_iota(jnp.int32, (N, N), 1)
    weight[...] = screened(squares(row) + squares(jnp.full((N, N), me, jnp.int32)) + squares(column))

    load_own.wait()
    load_tables.wait()
    high, low, high_t, low_t = (tables[i] for i in range(4))

    def right_of(a, b):
        both = jnp.concatenate([a, b], axis=1)
        return jnp.concatenate([both, both], axis=0)

    def left_of(a, b):
        both = jnp.concatenate([a, b], axis=0)
        return jnp.concatenate([both, both], axis=1)

    def forward(chunk, densities):
        first = times(jnp.concatenate(densities, axis=0), right_of(high_t, low_t))
        side = jnp.concatenate([first[p * N : (p + 1) * N] for p in range(len(densities))], axis=1)
        scatter(out1, chunk, applied(left_of(high, low), side))

    def middle(chunk):
        spectrum = applied(left_of(high, low), gather(in1, chunk))
        spectrum = spectrum * jnp.concatenate([weight[...]] * CHUNKS[chunk][1], axis=1)
        scatter(out2, chunk, applied(left_of(high_t, low_t), spectrum))

    def backward(chunk):
        rows = CHUNKS[chunk][1]
        side = applied(left_of(high_t, low_t), gather(in2, chunk))
        stack = jnp.concatenate([side[:, p * N : (p + 1) * N] for p in range(rows)], axis=0)
        field = times(stack, right_of(high, low))
        return [field[p * N : (p + 1) * N] for p in range(rows)]

    forward(0, [own[0] * own[0], own[0] * own[1], own[1] * own[1]])

    pl.semaphore_wait(barrier, N)
    shift = pltpu.make_async_remote_copy(
        src_ref=own, dst_ref=other, send_sem=near_send, recv_sem=near_recv, device_id=following, device_id_type=LOGICAL
    )
    shift.start()
    sends(out1, in1, 0)
    shift.wait_recv()
    forward(1, [own[0] * other[0], own[0] * other[1], own[1] * other[0], own[1] * other[1]])
    sends(out1, in1, 1)
    for chunk in range(2):
        whole(out1, in1, chunk).wait_recv()
        middle(chunk)
        returns(out2, in2, 2 + chunk)
    whole(out2, in2, 2).wait_recv()
    field = backward(0)
    own_part = [field[0] * own[0] + field[1] * own[1], field[1] * own[0] + field[2] * own[1]]
    whole(out2, in2, 3).wait_recv()
    field = backward(1)
    out_ref[0] = (own_part[0] + (field[0] * other[0] + field[1] * other[1]))
    out_ref[1] = (own_part[1] + (field[2] * other[0] + field[3] * other[1]))
    shift.wait_send()
    for number in range(4):
        source, target = ((out1, in1), (out2, in2))[number // 2]
        whole(source, target, number).wait_send()


def body(orbitals):
    plane = pltpu.VMEM((N, 8, N), jnp.float32)
    pair = pltpu.VMEM((2, N, N), jnp.float32)
    result = pl.pallas_call(
        kernel,
        out_shape=pltpu.VMEM((2, N, N), jnp.float32),
        in_specs=[pl.BlockSpec(memory_space=pltpu.HBM)] * 2,
        out_specs=pl.BlockSpec(memory_space=pltpu.VMEM),
        scratch_shapes=[
            pair,
            pair,
            pltpu.VMEM((4, N, N), jnp.bfloat16),
            plane,
            plane,
            plane,
            plane,
            pltpu.VMEM((N, N), jnp.float32),
            pltpu.SemaphoreType.DMA((2,)),
            pltpu.SemaphoreType.DMA,
            pltpu.SemaphoreType.DMA,
            pltpu.SemaphoreType.DMA((4,)),
            pltpu.SemaphoreType.DMA((4,)),
        ],
        compiler_params=pltpu.CompilerParams(collective_id=0, has_side_effects=True),
        name="exchange",
    )(orbitals.reshape(2, N, N), jnp.asarray(basis()))
    return -result.reshape(orbitals.shape)


def solution(mesh):
    placed = P("band", "slab", None, None)
    return jax.shard_map(body, mesh=mesh, in_specs=(placed,), out_specs=placed, check_vma=False)
```
